32 devices in a mesh: dp: 8 (over y, x, core), seq: 4 (over z).
Axes of the slice: x: 2, y: 2, z: 4, core: 2. Of those that a mesh axis runs over, the one named last changes fastest.
Arguments:
- img_q_raw: bfloat16 [8, 512, 1536], P('dp', 'seq'), may hold values from -12 to 12
- img_k_raw: bfloat16 [8, 512, 1536], P('dp', 'seq'), may hold values from -6 to 6
- img_v: bfloat16 [8, 512, 1536], P('dp', 'seq'), may hold values from -6 to 6
- img_dout: bfloat16 [8, 512, 1536], P('dp', 'seq'), may hold values from -6 to 6
- txt_q_raw: bfloat16 [8, 64, 1536], P('dp', 'seq'), may hold values from -6 to 6
- txt_k_raw: bfloat16 [8, 64, 1536], P('dp'), may hold values from -6 to 6
- txt_v: bfloat16 [8, 64, 1536], P('dp'), may hold values from -6 to 6
- txt_dout: bfloat16 [8, 64, 1536], P('dp', 'seq'), may hold values from -6 to 6
- q_gain: float32 [128], replicated, may hold values from 0.6 to 3.8
- k_gain: float32 [128], replicated, may hold values from 0.6 to 3.8
Outputs:
- img_dq: bfloat16 [8, 512, 1536], P('dp', 'seq')
- img_dk: bfloat16 [8, 512, 1536], P('dp', 'seq')
- img_dv: bfloat16 [8, 512, 1536], P('dp', 'seq')
- txt_dq: bfloat16 [8, 64, 1536], P('dp', 'seq')
- txt_dk: bfloat16 [8, 64, 1536], P('dp', 'seq')
- txt_dv: bfloat16 [8, 64, 1536], P('dp', 'seq')
- q_gain_grad: float32 [128], replicated
- k_gain_grad: float32 [128], replicated
The draws below stay inside these ranges and needn't reach their ends.
All inputs are finite; a program needn't handle non-finite values.
Results may differ from the reference program's by a relative error of at most 0.012.
The reference program's roundings to bfloat16 on the way count: a program that leaves them out, or rounds other values in their place, can miss the bound.
Values may be sent and summed in bfloat16 or wider, within the bound.
A program may use at most 64 MiB of HBM per device.

```python
import jax
import jax.numpy as jnp
from jax import lax

HEADS = 12
HEAD_DIM = 128
IMG_DEV = 128
TEXT = 64
IMAGE = 512
BATCH = 8
N_SEQ = 4


def joint_image(key):
    base = jax.random.fold_in(key, 7)
    first_key, second_key = jax.random.split(base, 2)
    keys_image = jnp.clip(jax.random.normal(first_key, (BATCH, IMAGE, HEADS * HEAD_DIM), jnp.float32), -6.0, 6.0)
    queries = jnp.clip(jax.random.normal(second_key, (BATCH, IMAGE, HEADS * HEAD_DIM), jnp.float32), -6.0, 6.0)
    return (queries, keys_image)


def draw_img_q_raw(key, part):
    return joint_image(key)[0].astype(jnp.bfloat16)


def draw_img_k_raw(key, part):
    return joint_image(key)[1].astype(jnp.bfloat16)


def draw_q_gain(key, part):
    base = jax.random.fold_in(key, 11)
    return jax.random.uniform(base, (HEAD_DIM,), jnp.float32, 0.6, 1.4)


def draw_k_gain(key, part):
    base = jax.random.fold_in(key, 13)
    return jax.random.uniform(base, (HEAD_DIM,), jnp.float32, 0.6, 1.4)


def steps_of(key, shape, pieces, least, high):
    def one(dim, parts):
        heights = jax.random.uniform(jax.random.fold_in(jax.random.fold_in(key, 6), dim), (parts,), jnp.float32, least / len(pieces), high / len(pieces))
        return jnp.repeat(jnp.exp(heights), shape[dim] // parts).reshape((-1,) + (1,) * (len(shape) - dim - 1))

    factor_of = one(*pieces[0])
    for cut in pieces[1:]:
        factor_of = factor_of * one(*cut)
    return factor_of


def gaussian(key, extent, deviation, most, cuts=(), dtype=jnp.bfloat16):
    factor_of = steps_of(key, extent, cuts, -0.22, 0.18) if cuts else 1.0
    array = jax.random.normal(key, extent, jnp.float32) * deviation * factor_of
    return jnp.minimum(jnp.maximum(array, -most), most).astype(dtype)


def setup_inputs(seed: int = 0) -> dict:
    splits = jax.random.split(jax.random.key(seed), 11)
    return {
        "img_q_raw": draw_img_q_raw(jax.random.fold_in(splits[10], 71), 0),
        "img_k_raw": draw_img_k_raw(jax.random.fold_in(splits[10], 71), 0),
        "img_v": gaussian(splits[2], (BATCH, IMAGE, HEADS * HEAD_DIM), 1.0, 6.0, ((0, 8), (1, 4))),
        "img_dout": gaussian(splits[3], (BATCH, IMAGE, HEADS * HEAD_DIM), 1.0, 6.0, ((0, 8), (1, 4))),
        "txt_q_raw": gaussian(splits[4], (BATCH, TEXT, HEADS * HEAD_DIM), 1.0, 6.0, ((0, 8), (1, 4))),
        "txt_k_raw": gaussian(splits[5], (BATCH, TEXT, HEADS * HEAD_DIM), 1.0, 6.0, ((0, 8),)),
        "txt_v": gaussian(splits[6], (BATCH, TEXT, HEADS * HEAD_DIM), 1.0, 6.0, ((0, 8),)),
        "txt_dout": gaussian(splits[7], (BATCH, TEXT, HEADS * HEAD_DIM), 1.0, 6.0, ((0, 8), (1, 4))),
        "q_gain": draw_q_gain(jax.random.fold_in(splits[10], 71), 0),
        "k_gain": draw_k_gain(jax.random.fold_in(splits[10], 71), 0),
    }


epsilon = 1e-06

def normalize(source, norm_gain):
    values = source.astype(jnp.float32)
    inverse = lax.rsqrt(lax.optimization_barrier(jnp.mean(values * values, axis=-1, keepdims=True)) + epsilon)
    return values * inverse * norm_gain

def rounded(values):
    return lax.optimization_barrier(values.astype(jnp.bfloat16)).astype(jnp.float32)

def blocked(image_rows, text_rows):
    image_part = image_rows.reshape(N_SEQ, IMG_DEV, HEADS, HEAD_DIM)
    text_part = text_rows.reshape(N_SEQ, TEXT // N_SEQ, HEADS, HEAD_DIM)
    return jnp.concatenate([image_part, text_part], axis=1)

def sample(q_gain, k_gain, inputs):
    img_q, img_k, img_val, img_grad, txt_q, txt_k, txt_val, txt_grad = inputs
    query_src = blocked(img_q, txt_q).astype(jnp.float32)
    dout_f = blocked(img_grad, txt_grad).astype(jnp.float32)
    key_src = jnp.concatenate([img_k, txt_k], axis=0).reshape(IMAGE + TEXT, HEADS, HEAD_DIM).astype(jnp.float32)
    value_all = jnp.concatenate([img_val, txt_val], axis=0).reshape(IMAGE + TEXT, HEADS, HEAD_DIM).astype(jnp.float32)
    query_b = rounded(normalize(query_src, q_gain))
    key_b = rounded(normalize(key_src, k_gain))
    score_scale = HEAD_DIM ** (-0.5)
    scores = jnp.einsum('nqhd,khd->nhqk', query_b, key_b) * score_scale
    row_max = lax.optimization_barrier(jnp.max(scores, axis=-1, keepdims=True))
    shifted = scores - row_max
    log_total = jnp.log(lax.optimization_barrier(jnp.sum(jnp.exp(shifted), axis=-1, keepdims=True)))
    prob_full = jnp.exp(shifted - log_total)
    probs_b = rounded(prob_full)
    output_b = rounded(jnp.einsum('nhqk,khd->nqhd', probs_b, value_all))
    dprob = jnp.einsum('nqhd,khd->nhqk', dout_f, value_all)
    row_delta = jnp.transpose(lax.optimization_barrier(jnp.sum(dout_f * output_b, axis=-1)), (0, 2, 1))[..., None]
    dscore_b = rounded(prob_full * (dprob - row_delta) * score_scale)
    dquery = jnp.einsum('nhqk,khd->nqhd', dscore_b, key_b)
    dkey = lax.optimization_barrier(jnp.sum(rounded(jnp.einsum('nhqk,nqhd->nkhd', dscore_b, query_b)), axis=0))
    dvalue = lax.optimization_barrier(jnp.sum(rounded(jnp.einsum('nhqk,nqhd->nkhd', probs_b, dout_f)), axis=0))
    result_q, query_pull = jax.vjp(normalize, query_src, q_gain)
    dquery_src, dq_gain = query_pull(dquery)
    result_k, key_pull = jax.vjp(normalize, key_src, k_gain)
    dkey_src, dk_gain = key_pull(dkey)
    width_all = HEADS * HEAD_DIM
    dq_b = dquery_src.astype(jnp.bfloat16)
    image_dq = dq_b[:, :IMG_DEV].reshape(IMAGE, width_all)
    text_dq = dq_b[:, IMG_DEV:].reshape(TEXT, width_all)
    dk_b = dkey_src.reshape(IMAGE + TEXT, width_all).astype(jnp.bfloat16)
    dv_b = dvalue.reshape(IMAGE + TEXT, width_all).astype(jnp.bfloat16)
    return (image_dq, dk_b[:IMAGE], dv_b[:IMAGE], text_dq, dk_b[IMAGE:], dv_b[IMAGE:], dq_gain, dk_gain)

def reference(img_q_raw, img_k_raw, img_v, img_dout, txt_q_raw, txt_k_raw, txt_v, txt_dout, q_gain, k_gain):

    def per_sample(inputs):
        return sample(q_gain, k_gain, inputs)
    results = lax.map(per_sample, (img_q_raw, img_k_raw, img_v, img_dout, txt_q_raw, txt_k_raw, txt_v, txt_dout))
    return (results[0], results[1], results[2], results[3], results[4], results[5], lax.optimization_barrier(jnp.sum(results[6], axis=0)), lax.optimization_barrier(jnp.sum(results[7], axis=0)))
```

```python
import functools

import jax
import jax.numpy as jnp
from jax import lax
from jax.experimental import pallas as pl
from jax.experimental.pallas import tpu as pltpu
from jax.sharding import PartitionSpec as P

MESH = pl.DeviceIdType.MESH
HEAD_DIM = 128
EPSILON = 1e-06
VMEM_LIMIT = 24 * 1024 * 1024
F32 = jnp.float32
BF16 = jnp.bfloat16


def dot(a, b, contract):
    return lax.dot_general(a, b, ((contract[:1], contract[1:]), ((), ())), preferred_element_type=F32)


def inverse_rms(values):
    return lax.rsqrt(jnp.mean(values * values, axis=-1, keepdims=True) + EPSILON)


def norm_back(values, inverse, gain, upstream):
    unit = values * inverse
    lifted = upstream * gain
    mean = jnp.mean(lifted * unit, axis=-1, keepdims=True)
    return inverse * (lifted - unit * mean), upstream * unit


def ladder(dp):
    stages, stride = [], 1
    while stride < dp:
        radix = next(r for r in range(2, dp + 1) if (dp // stride) % r == 0)
        stages.append((stride, radix))
        stride *= radix
    return stages


def near_first(me, n, i):
    up = jnp.where(me + 1 + i < n, me + 1 + i, n - 2 - i)
    down = jnp.where(me - 1 - i >= 0, me - 1 - i, i + 1)
    return jnp.where(2 * me < n, up, down)


def far_first(me, n, i):
    up = jnp.where(n - 1 - i > me, n - 1 - i, n - 2 - i)
    down = jnp.where(i < me, i, i + 1)
    return jnp.where(2 * me < n, up, down)


def kernel(
    n, dp, heads,
    h_iq, h_ik, h_iv, h_idt, h_tq, h_tk, h_tv, h_td, h_qg, h_kg,
    y, total,
    x, tk, tv, gains, r, g, kc, vc, knb, dka, dva, gsum, dpbuf, sqbuf,
    ins, fs, fr, bs, br, gs, gr, tokens,
):
    me = lax.axis_index("seq")
    my_dp = lax.axis_index("dp")
    img, txt, text = h_iq.shape[0], h_tq.shape[0], h_tk.shape[0]
    block = img + txt
    sent = 2 * block + 2 * img
    back = 3 * block
    image = img * n
    stages = ladder(dp)
    has_left, has_right = me > 0, me < n - 1

    def col(owner, h):
        return pl.ds(pl.multiple_of((owner * heads + h) * HEAD_DIM, HEAD_DIM), HEAD_DIM)

    def rows(start, size):
        return pl.ds(pl.multiple_of(start, 16), size)

    def peers(stage):
        stride, radix = stages[stage]
        digit = lax.rem(lax.div(my_dp, stride), radix)
        return digit, [my_dp + (lax.rem(digit + s, radix) - digit) * stride for s in range(1, radix)]

    at = 0
    loads = []
    for src, size in ((h_iq, img), (h_tq, txt), (h_ik, img), (h_iv, img), (h_idt, img), (h_td, txt)):
        loads.append(pltpu.make_async_copy(src, x.at[pl.ds(at, size)], ins.at[0]))
        at += size
    loads.append(pltpu.make_async_copy(h_tk, tk, ins.at[1]))
    loads.append(pltpu.make_async_copy(h_tv, tv, ins.at[2]))
    loads.append(pltpu.make_async_copy(h_qg, gains.at[pl.ds(0, 1)], ins.at[3]))
    loads.append(pltpu.make_async_copy(h_kg, gains.at[pl.ds(1, 1)], ins.at[3]))
    barrier = pltpu.get_barrier_semaphore()

    @pl.when(has_left)
    def _():
        pl.semaphore_signal(barrier, inc=1, device_id={"seq": me - 1}, device_id_type=MESH)

    @pl.when(has_right)
    def _():
        pl.semaphore_signal(barrier, inc=1, device_id={"seq": me + 1}, device_id_type=MESH)

    greeted = 0
    for stage in range(len(stages)):
        for peer in peers(stage)[1]:
            pl.semaphore_signal(barrier, inc=1, device_id={"dp": peer}, device_id_type=MESH)
            greeted += 1
    for load in loads:
        load.start()
    pl.semaphore_wait(barrier, greeted + jnp.where(has_left, 1, 0) + jnp.where(has_right, 1, 0))

    def token(side, k, target):
        pl.semaphore_signal(tokens.at[side, k], inc=1, device_id={"seq": target}, device_id_type=MESH)

    @pl.when(has_left & has_right)
    def _():
        token(0, 0, me - 1)
        token(1, 0, me + 1)

    pltpu.make_async_copy(x, x, ins.at[0]).wait()

    def forward_copy(h, target):
        return pltpu.make_async_remote_copy(
            src_ref=x.at[:, col(target, h)], dst_ref=r.at[h, rows(me * sent, sent)],
            send_sem=fs.at[0], recv_sem=fr.at[h],
            device_id={"seq": target}, device_id_type=MESH,
        )

    first = near_first(me, n, 0)
    forward_copy(0, first).start()
    for k in range(n - 2):
        @pl.when(me < n - 2 - k)
        def _():
            pl.semaphore_wait(tokens.at[0, k], 1)

            @pl.when(has_left)
            def _():
                token(0, k + 1, me - 1)

        @pl.when(me > k + 1)
        def _():
            pl.semaphore_wait(tokens.at[1, k], 1)

            @pl.when(has_right)
            def _():
                token(1, k + 1, me + 1)

    for i in range(1, n - 1):
        forward_copy(0, near_first(me, n, i)).start()

    def send_head(h, carry):
        for i in range(n - 1):
            forward_copy(h, near_first(me, n, i)).start()
        return carry

    lax.fori_loop(1, heads, send_head, 0)

    def own_head(h, carry):
        r[h, rows(me * sent, sent)] = x[:, col(me, h)]
        return carry

    lax.fori_loop(0, heads, own_head, 0)
    gsum[...] = jnp.zeros_like(gsum)
    pltpu.make_async_copy(tk, tk, ins.at[1]).wait()
    pltpu.make_async_copy(tv, tv, ins.at[2]).wait()
    pltpu.make_async_copy(gains, gains, ins.at[3]).wait()

    def back_copy(h, target):
        return pltpu.make_async_remote_copy(
            src_ref=g.at[h, rows(target * back, back)], dst_ref=y.at[:, col(me, h)],
            send_sem=bs.at[0], recv_sem=br.at[0],
            device_id={"seq": target}, device_id_type=MESH,
        )

    def send_back(h):
        for i in range(n - 1):
            back_copy(h, far_first(me, n, i)).start()
        y[:, col(me, h)] = g[h, rows(me * back, back)]

    qg = gains[0:1]
    kg = gains[1:2]
    scale = HEAD_DIM ** (-0.5)

    def head(h, carry):
        rest = r.at[h, pl.ds(0, (n - 1) * sent)]
        pltpu.make_async_copy(rest, rest, fr.at[h]).wait()
        for j in range(n):
            kc[j * img:(j + 1) * img] = r[h, j * sent + block:j * sent + block + img]
            vc[j * img:(j + 1) * img] = r[h, j * sent + block + img:j * sent + block + 2 * img]
        kc[image:image + text] = tk[:, col(me, h)]
        vc[image:image + text] = tv[:, col(me, h)]
        key_src = kc[...].astype(F32)
        key_inv = inverse_rms(key_src)
        knb[...] = (key_src * key_inv * kg).astype(BF16)
        dka[...] = jnp.zeros_like(dka)
        dva[...] = jnp.zeros_like(dva)

        def one_block(j, inner):
            query_src = r[h, rows(j * sent, block)].astype(F32)
            query_inv = inverse_rms(query_src)
            qn = (query_src * query_inv * qg).astype(BF16)
            kn = knb[...]
            value = vc[...]
            dout = r[h, rows(j * sent + block + 2 * img, block)]
            scores = dot(qn, kn, (1, 1)) * scale
            exps = jnp.exp(scores - jnp.max(scores, axis=-1, keepdims=True))
            prob = exps * (1.0 / jnp.sum(exps, axis=-1, keepdims=True))
            prob_b = prob.astype(BF16)
            output = dot(prob_b, value, (1, 0)).astype(BF16)
            dprob = dot(dout, value, (1, 1))
            delta = jnp.sum(dout.astype(F32) * output.astype(F32), axis=-1, keepdims=True)
            dscore = (prob * (dprob - delta) * scale).astype(BF16)
            dqn = dot(dscore, kn, (1, 0))
            dka[...] += dot(dscore, qn, (0, 0)).astype(BF16).astype(F32)
            dva[...] += dot(prob_b, dout, (0, 0)).astype(BF16).astype(F32)
            dq, term = norm_back(query_src, query_inv, qg, dqn)
            g[h, rows(j * back, block)] = dq.astype(BF16)
            gsum[0:1, :] += jnp.sum(term, axis=0, keepdims=True)
            return inner

        lax.fori_loop(0, n, one_block, 0)
        dk, term = norm_back(key_src, key_inv, kg, dka[...])
        gsum[1:2, :] += jnp.sum(term, axis=0, keepdims=True)
        for part, grad in ((1, dk.astype(BF16)), (2, dva[...].astype(BF16))):
            for j in range(n):
                start = j * back + part * block
                g[h, start:start + img] = grad[j * img:(j + 1) * img]
                g[h, start + img:start + block] = grad[image + j * txt:image + (j + 1) * txt]

        @pl.when(h < heads - 1)
        def _():
            send_back(h)

        return carry

    lax.fori_loop(0, heads, head, 0)

    partial = gsum[...]
    base = 0
    for stage, (stride, radix) in enumerate(stages):
        digit, others = peers(stage)
        slot = dpbuf.at[base + digit]
        slot[...] = partial
        for peer in others:
            pltpu.make_async_remote_copy(
                src_ref=slot, dst_ref=slot, send_sem=gs.at[stage], recv_sem=gr.at[stage],
                device_id={"dp": peer}, device_id_type=MESH,
            ).start()
        rest = dpbuf.at[pl.ds(base, radix - 1)]
        pltpu.make_async_copy(rest, rest, gr.at[stage]).wait()
        partial = jnp.sum(dpbuf[base:base + radix], axis=0)
        base += radix
    last = len(stages)
    sqbuf[me] = partial
    for i in range(n - 1):
        pltpu.make_async_remote_copy(
            src_ref=sqbuf.at[me], dst_ref=sqbuf.at[me], send_sem=gs.at[last], recv_sem=gr.at[last],
            device_id={"seq": far_first(me, n, i)}, device_id_type=MESH,
        ).start()
    send_back(heads - 1)

    base = 0
    for stage, (stride, radix) in enumerate(stages):
        rest = dpbuf.at[pl.ds(base, radix - 1)]
        pltpu.make_async_copy(rest, rest, gs.at[stage]).wait()
        base += radix
    out = x.at[:, pl.ds(0, (n - 1) * heads * HEAD_DIM)]
    pltpu.make_async_copy(out, out, fs.at[0]).wait()
    rest = sqbuf.at[pl.ds(0, n - 1)]
    pltpu.make_async_copy(rest, rest, gr.at[last]).wait()
    pltpu.make_async_copy(rest, rest, gs.at[last]).wait()
    total[...] = jnp.sum(sqbuf[...], axis=0)
    out = y.at[:, pl.ds(0, (n - 1) * heads * HEAD_DIM)]
    pltpu.make_async_copy(out, out, bs.at[0]).wait()
    pltpu.make_async_copy(out, out, br.at[0]).wait()


def hand_on(y, total, *refs):
    grads, gains, sems = refs[:6], refs[6:8], refs[8]
    at = 0
    stores = []
    for out in grads:
        stores.append(pltpu.make_async_copy(y.at[pl.ds(at, out.shape[0])], out, sems.at[0]))
        at += out.shape[0]
    for i, out in enumerate(gains):
        stores.append(pltpu.make_async_copy(total.at[pl.ds(i, 1)], out, sems.at[1]))
    for store in stores:
        store.start()
    pltpu.make_async_copy(y, y, sems.at[0]).wait()
    pltpu.make_async_copy(total, total, sems.at[1]).wait()


def local(n, dp, iq, ik, iv, idt, tq, tk, tv, td, q_gain, k_gain):
    img, width = iq.shape[1:]
    txt, text = tq.shape[1], tk.shape[1]
    heads = width // HEAD_DIM // n
    keys = img * n + text
    block = img + txt
    sent, back = 2 * block + 2 * img, 3 * block
    stages = ladder(dp)
    vmem = pl.BlockSpec(memory_space=pltpu.VMEM)
    hbm = pl.BlockSpec(memory_space=pltpu.HBM)
    out = pl.pallas_call(
        functools.partial(kernel, n, dp, heads),
        out_shape=(
            jax.ShapeDtypeStruct((back, width), BF16),
            jax.ShapeDtypeStruct((2, HEAD_DIM), F32),
        ),
        in_specs=[hbm] * 10,
        out_specs=(vmem, vmem),
        scratch_shapes=[
            pltpu.VMEM((sent, width), BF16),
            pltpu.VMEM((text, width), BF16),
            pltpu.VMEM((text, width), BF16),
            pltpu.VMEM((2, HEAD_DIM), F32),
            pltpu.VMEM((heads, n * sent, HEAD_DIM), BF16),
            pltpu.VMEM((heads, n * back, HEAD_DIM), BF16),
            pltpu.VMEM((keys, HEAD_DIM), BF16),
            pltpu.VMEM((keys, HEAD_DIM), BF16),
            pltpu.VMEM((keys, HEAD_DIM), BF16),
            pltpu.VMEM((keys, HEAD_DIM), F32),
            pltpu.VMEM((keys, HEAD_DIM), F32),
            pltpu.VMEM((2, HEAD_DIM), F32),
            pltpu.VMEM((sum(radix for _, radix in stages), 2, HEAD_DIM), F32),
            pltpu.VMEM((n, 2, HEAD_DIM), F32),
            pltpu.SemaphoreType.DMA((4,)),
            pltpu.SemaphoreType.DMA((1,)),
            pltpu.SemaphoreType.DMA((heads,)),
            pltpu.SemaphoreType.DMA((1,)),
            pltpu.SemaphoreType.DMA((1,)),
            pltpu.SemaphoreType.DMA((len(stages) + 1,)),
            pltpu.SemaphoreType.DMA((len(stages) + 1,)),
            pltpu.SemaphoreType.REGULAR((2, max(n - 1, 1))),
        ],
        compiler_params=pltpu.CompilerParams(
            collective_id=0, has_side_effects=True, vmem_limit_bytes=VMEM_LIMIT
        ),
    )(
        *(pltpu.with_memory_space_constraint(a, pltpu.HBM) for a in (
        iq[0], ik[0], iv[0], idt[0], tq[0], tk[0], tv[0], td[0],
        q_gain.reshape(1, HEAD_DIM), k_gain.reshape(1, HEAD_DIM)))
    )
    image, rest = (img, width), (txt, width)
    final = pl.pallas_call(
        hand_on,
        out_shape=tuple(jax.ShapeDtypeStruct(a, BF16) for a in (image, rest) * 3)
        + (jax.ShapeDtypeStruct((1, HEAD_DIM), F32),) * 2,
        in_specs=[vmem] * 2,
        out_specs=(hbm,) * 8,
        scratch_shapes=[pltpu.SemaphoreType.DMA((2,))],
        compiler_params=pltpu.CompilerParams(vmem_limit_bytes=VMEM_LIMIT),
    )(*out)
    order = (0, 2, 4, 1, 3, 5)
    return (*(final[i][None] for i in order), final[6][0], final[7][0])


def solution(mesh):
    split = P("dp", "seq", None)
    whole = P("dp", None, None)
    return jax.shard_map(
        functools.partial(local, mesh.shape["seq"], mesh.shape["dp"]),
        mesh=mesh,
        in_specs=(split, split, split, split, split, whole, whole, split, P(), P()),
        out_specs=(split,) * 6 + (P(), P()),
        check_vma=False,
    )
```

```python
import functools

import jax
import jax.numpy as jnp
from jax import lax
from jax.experimental import pallas as pl
from jax.experimental.pallas import tpu as pltpu
from jax.sharding import PartitionSpec as P

MESH = pl.DeviceIdType.MESH
HEAD_DIM = 128
EPSILON = 1e-06
VMEM_LIMIT = 24 * 1024 * 1024
F32 = jnp.float32
BF16 = jnp.bfloat16


def dot(a, b, contract):
    return lax.dot_general(a, b, ((contract[:1], contract[1:]), ((), ())), preferred_element_type=F32)


def inverse_rms(values):
    return lax.rsqrt(jnp.mean(values * values, axis=-1, keepdims=True) + EPSILON)


def norm_back(values, inverse, gain, upstream):
    unit = values * inverse
    lifted = upstream * gain
    mean = jnp.mean(lifted * unit, axis=-1, keepdims=True)
    return inverse * (lifted - unit * mean), upstream * unit


def ladder(dp):
    stages, stride = [], 1
    while stride < dp:
        radix = next(r for r in range(2, dp + 1) if (dp // stride) % r == 0)
        stages.append((stride, radix))
        stride *= radix
    return stages


def near_first(me, n, i):
    up = jnp.where(me + 1 + i < n, me + 1 + i, n - 2 - i)
    down = jnp.where(me - 1 - i >= 0, me - 1 - i, i + 1)
    return jnp.where(2 * me < n, up, down)


def far_first(me, n, i):
    up = jnp.where(n - 1 - i > me, n - 1 - i, n - 2 - i)
    down = jnp.where(i < me, i, i + 1)
    return jnp.where(2 * me < n, up, down)


def kernel(
    n, dp, heads,
    h_iq, h_ik, h_iv, h_idt, h_tq, h_tk, h_tv, h_td, h_qg, h_kg,
    y, total,
    x, tk, tv, gains, r, g, kc, vc, knb, dka, dva, gsum, dpbuf, sqbuf,
    ins, fs, fr, bs, br, gs, gr, tokens, column,
):
    me = lax.axis_index("seq")
    my_dp = lax.axis_index("dp")
    img, txt, text = h_iq.shape[0], h_tq.shape[0], h_tk.shape[0]
    block = img + txt
    sent = 2 * block + 2 * img
    back = 3 * block
    image = img * n
    stages = ladder(dp)
    has_left, has_right = me > 0, me < n - 1

    def col(owner, h):
        return pl.ds(pl.multiple_of((owner * heads + h) * HEAD_DIM, HEAD_DIM), HEAD_DIM)

    def rows(start, size):
        return pl.ds(pl.multiple_of(start, 16), size)

    def peers(stage):
        stride, radix = stages[stage]
        digit = lax.rem(lax.div(my_dp, stride), radix)
        return digit, [my_dp + (lax.rem(digit + s, radix) - digit) * stride for s in range(1, radix)]

    order = [near_first(me, n, i) for i in range(n - 1)] + [me]

    def band(i):
        return pl.ds(pl.multiple_of(order[i] * heads * HEAD_DIM, HEAD_DIM), heads * HEAD_DIM)

    def load_band(i):
        at = 0
        for src, size in ((h_iq, img), (h_tq, txt), (h_ik, img), (h_iv, img), (h_idt, img), (h_td, txt)):
            pltpu.make_async_copy(
                src.at[:, band(i)], x.at[pl.ds(at, size), band(i)], ins.at[i]
            ).start()
            at += size

    def wait_band(i):
        part = x.at[:, pl.ds(0, heads * HEAD_DIM)]
        pltpu.make_async_copy(part, part, ins.at[i]).wait()

    def small_loads():
        return (
            pltpu.make_async_copy(h_tk, tk, ins.at[n]),
            pltpu.make_async_copy(h_tv, tv, ins.at[n + 1]),
            pltpu.make_async_copy(h_qg, gains.at[pl.ds(0, 1)], ins.at[n + 2]),
            pltpu.make_async_copy(h_kg, gains.at[pl.ds(1, 1)], ins.at[n + 2]),
        )

    barrier = pltpu.get_barrier_semaphore()

    def tell(ref, axis, target):
        pl.semaphore_signal(ref, inc=1, device_id={axis: target}, device_id_type=MESH)

    @pl.when(has_right)
    def _():
        tell(barrier, "seq", me + 1)

    load_band(0)
    dp_peers = [peer for stage in range(len(stages)) for peer in peers(stage)[1]]

    @pl.when(me == 0)
    def _():
        for peer in dp_peers:
            tell(barrier, "dp", peer)

    for i in range(1, n):
        load_band(i)
    for load in small_loads():
        load.start()

    @pl.when(has_left)
    def _():
        pl.semaphore_wait(barrier, 1)
        tell(tokens.at[0, 0], "seq", me - 1)

    def forward_copy(h, target):
        return pltpu.make_async_remote_copy(
            src_ref=x.at[:, col(target, h)], dst_ref=r.at[h, rows(me * sent, sent)],
            send_sem=fs.at[0], recv_sem=fr.at[h],
            device_id={"seq": target}, device_id_type=MESH,
        )

    @pl.when(2 * me >= n)
    def _():
        wait_band(0)
        forward_copy(0, order[0]).start()

    for k in range(n - 1):
        @pl.when(me < n - 1 - k)
        def _():
            pl.semaphore_wait(tokens.at[0, k], 1)
            if k == 0:
                @pl.when(2 * me < n)
                def _():
                    wait_band(0)
                    forward_copy(0, order[0]).start()

                @pl.when(has_left)
                def _():
                    tell(tokens.at[1, 0], "seq", me + 1)

            if k < n - 2:
                @pl.when(has_left)
                def _():
                    tell(tokens.at[0, k + 1], "seq", me - 1)

    for k in range(n - 2):
        @pl.when(me > k + 1)
        def _():
            pl.semaphore_wait(tokens.at[1, k], 1)
            if k < n - 3:
                @pl.when(has_right)
                def _():
                    tell(tokens.at[1, k + 1], "seq", me + 1)

    for i in range(1, n - 1):
        wait_band(i)
        forward_copy(0, order[i]).start()

    def send_head(h, carry):
        for i in range(n - 1):
            forward_copy(h, order[i]).start()
        return carry

    lax.fori_loop(1, heads, send_head, 0)
    wait_band(n - 1)

    @pl.when(me == 0)
    def _():
        pl.semaphore_wait(barrier, len(dp_peers))
        for peer in dp_peers:
            tell(column.at[0], "dp", peer)
        pl.semaphore_wait(column.at[0], len(dp_peers))
        for target in range(1, n):
            tell(column.at[1], "seq", target)

    def own_head(h, carry):
        r[h, rows(me * sent, sent)] = x[:, col(me, h)]
        return carry

    lax.fori_loop(0, heads, own_head, 0)
    gsum[...] = jnp.zeros_like(gsum)
    pltpu.make_async_copy(tk, tk, ins.at[n]).wait()
    pltpu.make_async_copy(tv, tv, ins.at[n + 1]).wait()
    pltpu.make_async_copy(gains, gains, ins.at[n + 2]).wait()

    def back_copy(h, target):
        return pltpu.make_async_remote_copy(
            src_ref=g.at[h, rows(target * back, back)], dst_ref=y.at[:, col(me, h)],
            send_sem=bs.at[0], recv_sem=br.at[0],
            device_id={"seq": target}, device_id_type=MESH,
        )

    def send_back(h):
        for i in range(n - 1):
            back_copy(h, far_first(me, n, i)).start()

    def keep_own(h):
        y[:, col(me, h)] = g[h, rows(me * back, back)]

    qg = gains[0:1]
    kg = gains[1:2]
    scale = HEAD_DIM ** (-0.5)

    def head(h, carry):
        rest = r.at[h, pl.ds(0, (n - 1) * sent)]
        pltpu.make_async_copy(rest, rest, fr.at[h]).wait()
        for j in range(n):
            kc[j * img:(j + 1) * img] = r[h, j * sent + block:j * sent + block + img]
            vc[j * img:(j + 1) * img] = r[h, j * sent + block + img:j * sent + block + 2 * img]
        kc[image:image + text] = tk[:, col(me, h)]
        vc[image:image + text] = tv[:, col(me, h)]
        key_src = kc[...].astype(F32)
        key_inv = inverse_rms(key_src)
        knb[...] = (key_src * key_inv * kg).astype(BF16)
        dka[...] = jnp.zeros_like(dka)
        dva[...] = jnp.zeros_like(dva)

        def one_block(j, inner):
            query_src = r[h, rows(j * sent, block)].astype(F32)
            query_inv = inverse_rms(query_src)
            qn = (query_src * query_inv * qg).astype(BF16)
            kn = knb[...]
            value = vc[...]
            dout = r[h, rows(j * sent + block + 2 * img, block)]
            scores = dot(qn, kn, (1, 1)) * scale
            exps = jnp.exp(scores - jnp.max(scores, axis=-1, keepdims=True))
            prob = exps * (1.0 / jnp.sum(exps, axis=-1, keepdims=True))
            prob_b = prob.astype(BF16)
            output = dot(prob_b, value, (1, 0)).astype(BF16)
            dprob = dot(dout, value, (1, 1))
            delta = jnp.sum(dout.astype(F32) * output.astype(F32), axis=-1, keepdims=True)
            dscore = (prob * (dprob - delta) * scale).astype(BF16)
            dqn = dot(dscore, kn, (1, 0))
            dka[...] += dot(dscore, qn, (0, 0)).astype(BF16).astype(F32)
            dva[...] += dot(prob_b, dout, (0, 0)).astype(BF16).astype(F32)
            dq, term = norm_back(query_src, query_inv, qg, dqn)
            g[h, rows(j * back, block)] = dq.astype(BF16)
            gsum[0:1, :] += jnp.sum(term, axis=0, keepdims=True)
            return inner

        lax.fori_loop(0, n, one_block, 0)
        dk, term = norm_back(key_src, key_inv, kg, dka[...])
        gsum[1:2, :] += jnp.sum(term, axis=0, keepdims=True)
        for part, grad in ((1, dk.astype(BF16)), (2, dva[...].astype(BF16))):
            for j in range(n):
                start = j * back + part * block
                g[h, start:start + img] = grad[j * img:(j + 1) * img]
                g[h, start + img:start + block] = grad[image + j * txt:image + (j + 1) * txt]

        @pl.when(h < heads - 1)
        def _():
            send_back(h)

        keep_own(h)
        return carry

    lax.fori_loop(0, heads, head, 0)


    @pl.when(has_left)
    def _():
        pl.semaphore_wait(column.at[1], 1)

    partial = gsum[...]
    base = 0
    for stage, (stride, radix) in enumerate(stages):
        digit, others = peers(stage)
        slot = dpbuf.at[base + digit]
        slot[...] = partial
        for peer in others:
            pltpu.make_async_remote_copy(
                src_ref=slot, dst_ref=slot, send_sem=gs.at[stage], recv_sem=gr.at[stage],
                device_id={"dp": peer}, device_id_type=MESH,
            ).start()
        rest = dpbuf.at[pl.ds(base, radix - 1)]
        pltpu.make_async_copy(rest, rest, gr.at[stage]).wait()
        partial = jnp.sum(dpbuf[base:base + radix], axis=0)
        base += radix
    last = len(stages)
    sqbuf[me] = partial
    for i in range(n - 1):
        pltpu.make_async_remote_copy(
            src_ref=sqbuf.at[me], dst_ref=sqbuf.at[me], send_sem=gs.at[last], recv_sem=gr.at[last],
            device_id={"seq": far_first(me, n, i)}, device_id_type=MESH,
        ).start()
    for i in range(n - 1):
        back_copy(heads - 1, far_first(me, n, i)).start()

    base = 0
    for stage, (stride, radix) in enumerate(stages):
        rest = dpbuf.at[pl.ds(base, radix - 1)]
        pltpu.make_async_copy(rest, rest, gs.at[stage]).wait()
        base += radix
    out = x.at[:, pl.ds(0, (n - 1) * heads * HEAD_DIM)]
    pltpu.make_async_copy(out, out, fs.at[0]).wait()
    rest = sqbuf.at[pl.ds(0, n - 1)]
    pltpu.make_async_copy(rest, rest, gr.at[last]).wait()
    pltpu.make_async_copy(rest, rest, gs.at[last]).wait()
    total[...] = jnp.sum(sqbuf[...], axis=0)
    out = y.at[:, pl.ds(0, (n - 1) * heads * HEAD_DIM)]
    pltpu.make_async_copy(out, out, bs.at[0]).wait()
    pltpu.make_async_copy(out, out, br.at[0]).wait()


def hand_on(y, total, *refs):
    grads, gains, sems = refs[:6], refs[6:8], refs[8]
    at = 0
    stores = []
    for out in grads:
        stores.append(pltpu.make_async_copy(y.at[pl.ds(at, out.shape[0])], out, sems.at[0]))
        at += out.shape[0]
    for i, out in enumerate(gains):
        stores.append(pltpu.make_async_copy(total.at[pl.ds(i, 1)], out, sems.at[1]))
    for store in stores:
        store.start()
    pltpu.make_async_copy(y, y, sems.at[0]).wait()
    pltpu.make_async_copy(total, total, sems.at[1]).wait()


def local(n, dp, iq, ik, iv, idt, tq, tk, tv, td, q_gain, k_gain):
    img, width = iq.shape[1:]
    txt, text = tq.shape[1], tk.shape[1]
    heads = width // HEAD_DIM // n
    keys = img * n + text
    block = img + txt
    sent, back = 2 * block + 2 * img, 3 * block
    stages = ladder(dp)
    vmem = pl.BlockSpec(memory_space=pltpu.VMEM)
    hbm = pl.BlockSpec(memory_space=pltpu.HBM)
    out = pl.pallas_call(
        functools.partial(kernel, n, dp, heads),
        out_shape=(
            jax.ShapeDtypeStruct((back, width), BF16),
            jax.ShapeDtypeStruct((2, HEAD_DIM), F32),
        ),
        in_specs=[hbm] * 10,
        out_specs=(vmem, vmem),
        scratch_shapes=[
            pltpu.VMEM((sent, width), BF16),
            pltpu.VMEM((text, width), BF16),
            pltpu.VMEM((text, width), BF16),
            pltpu.VMEM((2, HEAD_DIM), F32),
            pltpu.VMEM((heads, n * sent, HEAD_DIM), BF16),
            pltpu.VMEM((heads, n * back, HEAD_DIM), BF16),
            pltpu.VMEM((keys, HEAD_DIM), BF16),
            pltpu.VMEM((keys, HEAD_DIM), BF16),
            pltpu.VMEM((keys, HEAD_DIM), BF16),
            pltpu.VMEM((keys, HEAD_DIM), F32),
            pltpu.VMEM((keys, HEAD_DIM), F32),
            pltpu.VMEM((2, HEAD_DIM), F32),
            pltpu.VMEM((sum(radix for _, radix in stages), 2, HEAD_DIM), F32),
            pltpu.VMEM((n, 2, HEAD_DIM), F32),
            pltpu.SemaphoreType.DMA((n + 3,)),
            pltpu.SemaphoreType.DMA((1,)),
            pltpu.SemaphoreType.DMA((heads,)),
            pltpu.SemaphoreType.DMA((1,)),
            pltpu.SemaphoreType.DMA((1,)),
            pltpu.SemaphoreType.DMA((len(stages) + 1,)),
            pltpu.SemaphoreType.DMA((len(stages) + 1,)),
            pltpu.SemaphoreType.REGULAR((2, n)),
            pltpu.SemaphoreType.REGULAR((2,)),
        ],
        compiler_params=pltpu.CompilerParams(
            collective_id=0, has_side_effects=True, vmem_limit_bytes=VMEM_LIMIT
        ),
    )(
        *(pltpu.with_memory_space_constraint(a, pltpu.HBM) for a in (
        iq[0], ik[0], iv[0], idt[0], tq[0], tk[0], tv[0], td[0],
        q_gain.reshape(1, HEAD_DIM), k_gain.reshape(1, HEAD_DIM)))
    )
    image, rest = (img, width), (txt, width)
    final = pl.pallas_call(
        hand_on,
        out_shape=tuple(jax.ShapeDtypeStruct(a, BF16) for a in (image, rest) * 3)
        + (jax.ShapeDtypeStruct((1, HEAD_DIM), F32),) * 2,
        in_specs=[vmem] * 2,
        out_specs=(hbm,) * 8,
        scratch_shapes=[pltpu.SemaphoreType.DMA((2,))],
        compiler_params=pltpu.CompilerParams(vmem_limit_bytes=VMEM_LIMIT),
    )(*out)
    order = (0, 2, 4, 1, 3, 5)
    return (*(final[i][None] for i in order), final[6][0], final[7][0])


def solution(mesh):
    split = P("dp", "seq", None)
    whole = P("dp", None, None)
    return jax.shard_map(
        functools.partial(local, mesh.shape["seq"], mesh.shape["dp"]),
        mesh=mesh,
        in_specs=(split, split, split, split, split, whole, whole, split, P(), P()),
        out_specs=(split,) * 6 + (P(), P()),
        check_vma=False,
    )
```

```python
import functools

import jax
import jax.numpy as jnp
from jax import lax
from jax.experimental import pallas as pl
from jax.experimental.pallas import tpu as pltpu
from jax.sharding import PartitionSpec as P

MESH = pl.DeviceIdType.MESH
HEAD_DIM = 128
EPSILON = 1e-06
VMEM_LIMIT = 24 * 1024 * 1024
F32 = jnp.float32
BF16 = jnp.bfloat16


def dot(a, b, contract):
    return lax.dot_general(a, b, ((contract[:1], contract[1:]), ((), ())), preferred_element_type=F32)


def inverse_rms(values):
    return lax.rsqrt(jnp.mean(values * values, axis=-1, keepdims=True) + EPSILON)


def norm_back(values, inverse, gain, upstream):
    unit = values * inverse
    lifted = upstream * gain
    mean = jnp.mean(lifted * unit, axis=-1, keepdims=True)
    return inverse * (lifted - unit * mean), upstream * unit


def ladder(dp):
    stages, stride = [], 1
    while stride < dp:
        left = dp // stride
        radix = max((r for r in range(2, 9) if left % r == 0), default=left)
        stages.append((stride, radix))
        stride *= radix
    return stages


def near_first(me, n, i):
    up = jnp.where(me + 1 + i < n, me + 1 + i, n - 2 - i)
    down = jnp.where(me - 1 - i >= 0, me - 1 - i, i + 1)
    return jnp.where(2 * me < n, up, down)


def cross_first(me, n, i):
    half = n // 2
    lower = me < half
    count = jnp.where(lower, n - half, half)
    own = jnp.where(lower, 0, half) + i - count
    return jnp.where(i < count, jnp.where(lower, half, 0) + i, jnp.where(own < me, own, own + 1))


def kernel(
    n, dp, heads,
    h_iq, h_ik, h_iv, h_idt, h_tq, h_tk, h_tv, h_td, h_qg, h_kg,
    y, total,
    x, tk, tv, gains, r, g, kc, vc, knb, dka, dva, gsum, dpbuf, sqbuf,
    ins, fs, fr, bs, br, gs, gr, tokens, column,
):
    me = lax.axis_index("seq")
    my_dp = lax.axis_index("dp")
    img, txt, text = h_iq.shape[0], h_tq.shape[0], h_tk.shape[0]
    block = img + txt
    sent = 2 * block + 2 * img
    back = 3 * block
    image = img * n
    stages = ladder(dp)
    has_left, has_right = me > 0, me < n - 1

    def col(owner, h):
        return pl.ds(pl.multiple_of((owner * heads + h) * HEAD_DIM, HEAD_DIM), HEAD_DIM)

    def rows(start, size):
        return pl.ds(pl.multiple_of(start, 16), size)

    def peers(stage):
        stride, radix = stages[stage]
        digit = lax.rem(lax.div(my_dp, stride), radix)
        return digit, [my_dp + (lax.rem(digit + s, radix) - digit) * stride for s in range(1, radix)]

    order = [near_first(me, n, i) for i in range(n - 1)] + [me]

    def band(i):
        return pl.ds(pl.multiple_of(order[i] * heads * HEAD_DIM, HEAD_DIM), heads * HEAD_DIM)

    def load_band(i):
        at = 0
        for part, (src, size) in enumerate(
            ((h_iq, img), (h_tq, txt), (h_ik, img), (h_iv, img), (h_idt, img), (h_td, txt))
        ):
            sem = ins.at[n + 3 if i == 0 and part == 0 else i]
            pltpu.make_async_copy(src.at[:, band(i)], x.at[pl.ds(at, size), band(i)], sem).start()
            at += size

    def wait_band(i):
        size = sent - img if i == 0 else sent
        part = x.at[pl.ds(0, size), pl.ds(0, heads * HEAD_DIM)]
        pltpu.make_async_copy(part, part, ins.at[i]).wait()

    def open_way():
        part = x.at[pl.ds(0, img), pl.ds(0, heads * HEAD_DIM)]
        pltpu.make_async_copy(part, part, ins.at[n + 3]).wait()
        forward_piece(order[0], 0, img).start()
        wait_band(0)
        forward_piece(order[0], img, sent - img).start()

    def small_loads():
        return (
            pltpu.make_async_copy(h_tk, tk, ins.at[n]),
            pltpu.make_async_copy(h_tv, tv, ins.at[n + 1]),
            pltpu.make_async_copy(h_qg, gains.at[pl.ds(0, 1)], ins.at[n + 2]),
            pltpu.make_async_copy(h_kg, gains.at[pl.ds(1, 1)], ins.at[n + 2]),
        )

    barrier = pltpu.get_barrier_semaphore()

    def tell(ref, axis, target):
        pl.semaphore_signal(ref, inc=1, device_id={axis: target}, device_id_type=MESH)

    @pl.when(has_right)
    def _():
        tell(barrier, "seq", me + 1)

    load_band(0)
    dp_peers = [peer for stage in range(len(stages)) for peer in peers(stage)[1]]

    @pl.when(me == 0)
    def _():
        for peer in dp_peers:
            tell(barrier, "dp", peer)

    @pl.when(has_left)
    def _():
        pl.semaphore_wait(barrier, 1)
        tell(tokens.at[0, 0], "seq", me - 1)

    for i in range(1, n):
        load_band(i)
    for load in small_loads():
        load.start()


    def forward_piece(target, start, size):
        return pltpu.make_async_remote_copy(
            src_ref=x.at[pl.ds(start, size), col(target, 0)],
            dst_ref=r.at[0, rows(me * sent + start, size)],
            send_sem=fs.at[0], recv_sem=fr.at[0],
            device_id={"seq": target}, device_id_type=MESH,
        )

    def forward_copy(h, target):
        return pltpu.make_async_remote_copy(
            src_ref=x.at[:, col(target, h)], dst_ref=r.at[h, rows(me * sent, sent)],
            send_sem=fs.at[0], recv_sem=fr.at[h],
            device_id={"seq": target}, device_id_type=MESH,
        )

    @pl.when(2 * me >= n)
    def _():
        open_way()

    for k in range(n - 1):
        @pl.when(me < n - 1 - k)
        def _():
            pl.semaphore_wait(tokens.at[0, k], 1)
            if k == 0:
                @pl.when(2 * me < n)
                def _():
                    open_way()

                @pl.when(has_left)
                def _():
                    tell(tokens.at[1, 0], "seq", me + 1)

            if k < n - 2:
                @pl.when(has_left)
                def _():
                    tell(tokens.at[0, k + 1], "seq", me - 1)

    for k in range(n - 2):
        @pl.when(me > k + 1)
        def _():
            pl.semaphore_wait(tokens.at[1, k], 1)
            if k < n - 3:
                @pl.when(has_right)
                def _():
                    tell(tokens.at[1, k + 1], "seq", me + 1)

    for i in range(1, n - 1):
        wait_band(i)
        forward_copy(0, order[i]).start()

    def send_head(h, carry):
        for i in range(n - 1):
            forward_copy(h, order[i]).start()
        return carry

    lax.fori_loop(1, heads, send_head, 0)
    wait_band(n - 1)

    @pl.when(me == 0)
    def _():
        pl.semaphore_wait(barrier, len(dp_peers))
        for peer in dp_peers:
            tell(column.at[0], "dp", peer)
        pl.semaphore_wait(column.at[0], len(dp_peers))
        for target in range(1, n):
            tell(column.at[1], "seq", target)

    def own_head(h, carry):
        r[h, rows(me * sent, sent)] = x[:, col(me, h)]
        return carry

    lax.fori_loop(0, heads, own_head, 0)
    gsum[...] = jnp.zeros_like(gsum)
    pltpu.make_async_copy(tk, tk, ins.at[n]).wait()
    pltpu.make_async_copy(tv, tv, ins.at[n + 1]).wait()
    pltpu.make_async_copy(gains, gains, ins.at[n + 2]).wait()

    def back_copy(h, target):
        return pltpu.make_async_remote_copy(
            src_ref=g.at[h, rows(target * back, back)], dst_ref=y.at[:, col(me, h)],
            send_sem=bs.at[0], recv_sem=br.at[0],
            device_id={"seq": target}, device_id_type=MESH,
        )

    def send_back(h):
        for i in range(n - 1):
            @pl.when((i != 1) | (h < heads - 2))
            def _():
                back_copy(h, cross_first(me, n, i)).start()

    def keep_own(h):
        y[:, col(me, h)] = g[h, rows(me * back, back)]

    qg = gains[0:1]
    kg = gains[1:2]
    scale = HEAD_DIM ** (-0.5)

    def head(h, carry):
        rest = r.at[h, pl.ds(0, (n - 1) * sent)]
        pltpu.make_async_copy(rest, rest, fr.at[h]).wait()
        for j in range(n):
            kc[j * img:(j + 1) * img] = r[h, j * sent + block:j * sent + block + img]
            vc[j * img:(j + 1) * img] = r[h, j * sent + block + img:j * sent + block + 2 * img]
        kc[image:image + text] = tk[:, col(me, h)]
        vc[image:image + text] = tv[:, col(me, h)]
        key_src = kc[...].astype(F32)
        key_inv = inverse_rms(key_src)
        knb[...] = (key_src * key_inv * kg).astype(BF16)
        dka[...] = jnp.zeros_like(dka)
        dva[...] = jnp.zeros_like(dva)

        def one_block(j, inner):
            query_src = r[h, rows(j * sent, block)].astype(F32)
            query_inv = inverse_rms(query_src)
            qn = (query_src * query_inv * qg).astype(BF16)
            kn = knb[...]
            value = vc[...]
            dout = r[h, rows(j * sent + block + 2 * img, block)]
            scores = dot(qn, kn, (1, 1)) * scale
            exps = jnp.exp(scores - jnp.max(scores, axis=-1, keepdims=True))
            prob = exps * (1.0 / jnp.sum(exps, axis=-1, keepdims=True))
            prob_b = prob.astype(BF16)
            output = dot(prob_b, value, (1, 0)).astype(BF16)
            dprob = dot(dout, value, (1, 1))
            delta = jnp.sum(dout.astype(F32) * output.astype(F32), axis=-1, keepdims=True)
            dscore = (prob * (dprob - delta) * scale).astype(BF16)
            dqn = dot(dscore, kn, (1, 0))
            dka[...] += dot(dscore, qn, (0, 0)).astype(BF16).astype(F32)
            dva[...] += dot(prob_b, dout, (0, 0)).astype(BF16).astype(F32)
            dq, term = norm_back(query_src, query_inv, qg, dqn)
            g[h, rows(j * back, block)] = dq.astype(BF16)
            gsum[0:1, :] += jnp.sum(term, axis=0, keepdims=True)
            return inner

        lax.fori_loop(0, n, one_block, 0)
        dk, term = norm_back(key_src, key_inv, kg, dka[...])
        gsum[1:2, :] += jnp.sum(term, axis=0, keepdims=True)
        for part, grad in ((1, dk.astype(BF16)), (2, dva[...].astype(BF16))):
            for j in range(n):
                start = j * back + part * block
                g[h, start:start + img] = grad[j * img:(j + 1) * img]
                g[h, start + img:start + block] = grad[image + j * txt:image + (j + 1) * txt]

        @pl.when(h < heads - 1)
        def _():
            send_back(h)

        keep_own(h)
        return carry

    lax.fori_loop(0, heads, head, 0)


    back_copy(heads - 1, cross_first(me, n, 0)).start()

    @pl.when(has_left)
    def _():
        pl.semaphore_wait(column.at[1], 1)

    partial = gsum[...]
    base = 0
    for stage, (stride, radix) in enumerate(stages):
        digit, others = peers(stage)
        slot = dpbuf.at[base + digit]
        slot[...] = partial
        for peer in others:
            pltpu.make_async_remote_copy(
                src_ref=slot, dst_ref=slot, send_sem=gs.at[stage], recv_sem=gr.at[stage],
                device_id={"dp": peer}, device_id_type=MESH,
            ).start()
        rest = dpbuf.at[pl.ds(base, radix - 1)]
        pltpu.make_async_copy(rest, rest, gr.at[stage]).wait()
        partial = jnp.sum(dpbuf[base:base + radix], axis=0)
        base += radix
    last = len(stages)
    sqbuf[me] = partial
    for i in range(n - 1):
        pltpu.make_async_remote_copy(
            src_ref=sqbuf.at[me], dst_ref=sqbuf.at[me], send_sem=gs.at[last], recv_sem=gr.at[last],
            device_id={"seq": cross_first(me, n, i)}, device_id_type=MESH,
        ).start()

    if heads > 1 and n > 2:
        back_copy(heads - 2, cross_first(me, n, 1)).start()

    for i in range(1, n - 1):
        back_copy(heads - 1, cross_first(me, n, i)).start()

    base = 0
    for stage, (stride, radix) in enumerate(stages):
        rest = dpbuf.at[pl.ds(base, radix - 1)]
        pltpu.make_async_copy(rest, rest, gs.at[stage]).wait()
        base += radix
    out = x.at[:, pl.ds(0, (n - 1) * heads * HEAD_DIM)]
    pltpu.make_async_copy(out, out, fs.at[0]).wait()
    rest = sqbuf.at[pl.ds(0, n - 1)]
    pltpu.make_async_copy(rest, rest, gr.at[last]).wait()
    pltpu.make_async_copy(rest, rest, gs.at[last]).wait()
    total[...] = jnp.sum(sqbuf[...], axis=0)
    out = y.at[:, pl.ds(0, (n - 1) * heads * HEAD_DIM)]
    pltpu.make_async_copy(out, out, bs.at[0]).wait()
    pltpu.make_async_copy(out, out, br.at[0]).wait()


def hand_on(y, total, *refs):
    grads, gains, sems = refs[:6], refs[6:8], refs[8]
    at = 0
    stores = []
    for out in grads:
        stores.append(pltpu.make_async_copy(y.at[pl.ds(at, out.shape[0])], out, sems.at[0]))
        at += out.shape[0]
    for i, out in enumerate(gains):
        stores.append(pltpu.make_async_copy(total.at[pl.ds(i, 1)], out, sems.at[1]))
    for store in stores:
        store.start()
    pltpu.make_async_copy(y, y, sems.at[0]).wait()
    pltpu.make_async_copy(total, total, sems.at[1]).wait()


def local(n, dp, iq, ik, iv, idt, tq, tk, tv, td, q_gain, k_gain):
    img, width = iq.shape[1:]
    txt, text = tq.shape[1], tk.shape[1]
    heads = width // HEAD_DIM // n
    keys = img * n + text
    block = img + txt
    sent, back = 2 * block + 2 * img, 3 * block
    stages = ladder(dp)
    vmem = pl.BlockSpec(memory_space=pltpu.VMEM)
    hbm = pl.BlockSpec(memory_space=pltpu.HBM)
    out = pl.pallas_call(
        functools.partial(kernel, n, dp, heads),
        out_shape=(
            jax.ShapeDtypeStruct((back, width), BF16),
            jax.ShapeDtypeStruct((2, HEAD_DIM), F32),
        ),
        in_specs=[hbm] * 10,
        out_specs=(vmem, vmem),
        scratch_shapes=[
            pltpu.VMEM((sent, width), BF16),
            pltpu.VMEM((text, width), BF16),
            pltpu.VMEM((text, width), BF16),
            pltpu.VMEM((2, HEAD_DIM), F32),
            pltpu.VMEM((heads, n * sent, HEAD_DIM), BF16),
            pltpu.VMEM((heads, n * back, HEAD_DIM), BF16),
            pltpu.VMEM((keys, HEAD_DIM), BF16),
            pltpu.VMEM((keys, HEAD_DIM), BF16),
            pltpu.VMEM((keys, HEAD_DIM), BF16),
            pltpu.VMEM((keys, HEAD_DIM), F32),
            pltpu.VMEM((keys, HEAD_DIM), F32),
            pltpu.VMEM((2, HEAD_DIM), F32),
            pltpu.VMEM((sum(radix for _, radix in stages), 2, HEAD_DIM), F32),
            pltpu.VMEM((n, 2, HEAD_DIM), F32),
            pltpu.SemaphoreType.DMA((n + 4,)),
            pltpu.SemaphoreType.DMA((1,)),
            pltpu.SemaphoreType.DMA((heads,)),
            pltpu.SemaphoreType.DMA((1,)),
            pltpu.SemaphoreType.DMA((1,)),
            pltpu.SemaphoreType.DMA((len(stages) + 1,)),
            pltpu.SemaphoreType.DMA((len(stages) + 1,)),
            pltpu.SemaphoreType.REGULAR((2, n)),
            pltpu.SemaphoreType.REGULAR((2,)),
        ],
        compiler_params=pltpu.CompilerParams(
            collective_id=0, has_side_effects=True, vmem_limit_bytes=VMEM_LIMIT
        ),
    )(
        *(pltpu.with_memory_space_constraint(a, pltpu.HBM) for a in (
        iq[0], ik[0], iv[0], idt[0], tq[0], tk[0], tv[0], td[0],
        q_gain.reshape(1, HEAD_DIM), k_gain.reshape(1, HEAD_DIM)))
    )
    image, rest = (img, width), (txt, width)
    final = pl.pallas_call(
        hand_on,
        out_shape=tuple(jax.ShapeDtypeStruct(a, BF16) for a in (image, rest) * 3)
        + (jax.ShapeDtypeStruct((1, HEAD_DIM), F32),) * 2,
        in_specs=[vmem] * 2,
        out_specs=(hbm,) * 8,
        scratch_shapes=[pltpu.SemaphoreType.DMA((2,))],
        compiler_params=pltpu.CompilerParams(vmem_limit_bytes=VMEM_LIMIT),
    )(*out)
    order = (0, 2, 4, 1, 3, 5)
    return (*(final[i][None] for i in order), final[6][0], final[7][0])


def solution(mesh):
    split = P("dp", "seq", None)
    whole = P("dp", None, None)
    return jax.shard_map(
        functools.partial(local, mesh.shape["seq"], mesh.shape["dp"]),
        mesh=mesh,
        in_specs=(split, split, split, split, split, whole, whole, split, P(), P()),
        out_specs=(split,) * 6 + (P(), P()),
        check_vma=False,
    )
```

```python
import functools

import jax
import jax.numpy as jnp
from jax import lax
from jax.experimental import pallas as pl
from jax.experimental.pallas import tpu as pltpu
from jax.sharding import PartitionSpec as P

MESH = pl.DeviceIdType.MESH
HEAD_DIM = 128
EPSILON = 1e-06
VMEM_LIMIT = 24 * 1024 * 1024
F32 = jnp.float32
BF16 = jnp.bfloat16


def dot(a, b, contract):
    return lax.dot_general(a, b, ((contract[:1], contract[1:]), ((), ())), preferred_element_type=F32)


def inverse_rms(values):
    return lax.rsqrt(jnp.mean(values * values, axis=-1, keepdims=True) + EPSILON)


def norm_back(values, inverse, gain, upstream):
    unit = values * inverse
    lifted = upstream * gain
    mean = jnp.mean(lifted * unit, axis=-1, keepdims=True)
    return inverse * (lifted - unit * mean), upstream * unit


def ladder(dp):
    stages, stride = [], 1
    while stride < dp:
        left = dp // stride
        radix = max((r for r in range(2, 9) if left % r == 0), default=left)
        stages.append((stride, radix))
        stride *= radix
    return stages


def near_first(me, n, i):
    up = jnp.where(me + 1 + i < n, me + 1 + i, n - 2 - i)
    down = jnp.where(me - 1 - i >= 0, me - 1 - i, i + 1)
    return jnp.where(2 * me < n, up, down)


def cross_first(me, n, i):
    half = n // 2
    lower = me < half
    count = jnp.where(lower, n - half, half)
    own = jnp.where(lower, 0, half) + i - count
    return jnp.where(i < count, jnp.where(lower, half, 0) + i, jnp.where(own < me, own, own + 1))


def kernel(
    n, dp, heads,
    h_iq, h_ik, h_iv, h_idt, h_tq, h_tk, h_tv, h_td, h_qg, h_kg,
    y, total,
    x, tk, tv, gains, r, g, kc, vc, knb, dka, dva, gsum, dpbuf, sqbuf,
    ins, fs, fr, bs, br, gs, gr, tokens, column,
):
    me = lax.axis_index("seq")
    my_dp = lax.axis_index("dp")
    img, txt, text = h_iq.shape[0], h_tq.shape[0], h_tk.shape[0]
    block = img + txt
    sent = 2 * block + 2 * img
    back = 3 * block
    image = img * n
    stages = ladder(dp)
    has_left, has_right = me > 0, me < n - 1

    def col(owner, h):
        return pl.ds(pl.multiple_of((owner * heads + h) * HEAD_DIM, HEAD_DIM), HEAD_DIM)

    def rows(start, size):
        return pl.ds(pl.multiple_of(start, 16), size)

    def peers(stage):
        stride, radix = stages[stage]
        digit = lax.rem(lax.div(my_dp, stride), radix)
        return digit, [my_dp + (lax.rem(digit + s, radix) - digit) * stride for s in range(1, radix)]

    order = [near_first(me, n, i) for i in range(n - 1)]
    parts, at = [], 0
    for src, size in ((h_iq, img), (h_tq, txt), (h_ik, img), (h_iv, img), (h_idt, img), (h_td, txt)):
        parts.append((src, at, size))
        at += size
    loads = [pltpu.make_async_copy(src, x.at[pl.ds(at, size)], ins.at[0]) for src, at, size in parts]
    loads += [
        pltpu.make_async_copy(h_tk, tk, ins.at[1]),
        pltpu.make_async_copy(h_tv, tv, ins.at[2]),
        pltpu.make_async_copy(h_qg, gains.at[pl.ds(0, 1)], ins.at[3]),
        pltpu.make_async_copy(h_kg, gains.at[pl.ds(1, 1)], ins.at[3]),
    ]
    barrier = pltpu.get_barrier_semaphore()

    def tell(ref, axis, target):
        pl.semaphore_signal(ref, inc=1, device_id={axis: target}, device_id_type=MESH)

    def first_copy():
        for src, at, size in parts:
            pltpu.make_async_remote_copy(
                src_ref=src.at[:, col(order[0], 0)], dst_ref=r.at[0, rows(me * sent + at, size)],
                send_sem=fs.at[0], recv_sem=fr.at[0],
                device_id={"seq": order[0]}, device_id_type=MESH,
            ).start()

    def forward_copy(h, target):
        return pltpu.make_async_remote_copy(
            src_ref=x.at[:, col(target, h)], dst_ref=r.at[h, rows(me * sent, sent)],
            send_sem=fs.at[0], recv_sem=fr.at[h],
            device_id={"seq": target}, device_id_type=MESH,
        )

    @pl.when(has_right)
    def _():
        tell(barrier, "seq", me + 1)

    @pl.when(has_left)
    def _():
        pl.semaphore_wait(barrier, 1)
        tell(tokens.at[0, 0], "seq", me - 1)

    @pl.when(2 * me >= n)
    def _():
        first_copy()

    for load in loads:
        load.start()
    dp_peers = [peer for stage in range(len(stages)) for peer in peers(stage)[1]]

    @pl.when(me == 0)
    def _():
        for peer in dp_peers:
            tell(barrier, "dp", peer)

    for k in range(n - 1):
        @pl.when(me < n - 1 - k)
        def _():
            pl.semaphore_wait(tokens.at[0, k], 1)
            if k == 0:
                @pl.when(2 * me < n)
                def _():
                    first_copy()

                @pl.when(has_left)
                def _():
                    tell(tokens.at[1, 0], "seq", me + 1)

            if k < n - 2:
                @pl.when(has_left)
                def _():
                    tell(tokens.at[0, k + 1], "seq", me - 1)

    for k in range(n - 2):
        @pl.when(me > k + 1)
        def _():
            pl.semaphore_wait(tokens.at[1, k], 1)
            if k < n - 3:
                @pl.when(has_right)
                def _():
                    tell(tokens.at[1, k + 1], "seq", me + 1)

    pltpu.make_async_copy(x, x, ins.at[0]).wait()
    for i in range(1, n - 1):
        forward_copy(0, order[i]).start()

    def send_head(h, carry):
        for i in range(n - 1):
            forward_copy(h, order[i]).start()
        return carry

    lax.fori_loop(1, heads, send_head, 0)

    @pl.when(me == 0)
    def _():
        pl.semaphore_wait(barrier, len(dp_peers))
        for peer in dp_peers:
            tell(column.at[0], "dp", peer)
        pl.semaphore_wait(column.at[0], len(dp_peers))
        for target in range(1, n):
            tell(column.at[1], "seq", target)

    def own_head(h, carry):
        r[h, rows(me * sent, sent)] = x[:, col(me, h)]
        return carry

    lax.fori_loop(0, heads, own_head, 0)
    gsum[...] = jnp.zeros_like(gsum)
    pltpu.make_async_copy(tk, tk, ins.at[1]).wait()
    pltpu.make_async_copy(tv, tv, ins.at[2]).wait()
    pltpu.make_async_copy(gains, gains, ins.at[3]).wait()

    def back_copy(h, target):
        return pltpu.make_async_remote_copy(
            src_ref=g.at[h, rows(target * back, back)], dst_ref=y.at[:, col(me, h)],
            send_sem=bs.at[0], recv_sem=br.at[0],
            device_id={"seq": target}, device_id_type=MESH,
        )

    def send_back(h):
        for i in range(n - 1):
            @pl.when((i != 1) | (h < heads - 2))
            def _():
                back_copy(h, cross_first(me, n, i)).start()

    def keep_own(h):
        y[:, col(me, h)] = g[h, rows(me * back, back)]

    qg = gains[0:1]
    kg = gains[1:2]
    scale = HEAD_DIM ** (-0.5)

    def head(h, carry):
        rest = r.at[h, pl.ds(0, (n - 1) * sent)]
        pltpu.make_async_copy(rest, rest, fr.at[h]).wait()
        for j in range(n):
            kc[j * img:(j + 1) * img] = r[h, j * sent + block:j * sent + block + img]
            vc[j * img:(j + 1) * img] = r[h, j * sent + block + img:j * sent + block + 2 * img]
        kc[image:image + text] = tk[:, col(me, h)]
        vc[image:image + text] = tv[:, col(me, h)]
        key_src = kc[...].astype(F32)
        key_inv = inverse_rms(key_src)
        knb[...] = (key_src * key_inv * kg).astype(BF16)
        dka[...] = jnp.zeros_like(dka)
        dva[...] = jnp.zeros_like(dva)

        def one_block(j, inner):
            query_src = r[h, rows(j * sent, block)].astype(F32)
            query_inv = inverse_rms(query_src)
            qn = (query_src * query_inv * qg).astype(BF16)
            kn = knb[...]
            value = vc[...]
            dout = r[h, rows(j * sent + block + 2 * img, block)]
            scores = dot(qn, kn, (1, 1)) * scale
            exps = jnp.exp(scores - jnp.max(scores, axis=-1, keepdims=True))
            prob = exps * (1.0 / jnp.sum(exps, axis=-1, keepdims=True))
            prob_b = prob.astype(BF16)
            output = dot(prob_b, value, (1, 0)).astype(BF16)
            dprob = dot(dout, value, (1, 1))
            delta = jnp.sum(dout.astype(F32) * output.astype(F32), axis=-1, keepdims=True)
            dscore = (prob * (dprob - delta) * scale).astype(BF16)
            dqn = dot(dscore, kn, (1, 0))
            dka[...] += dot(dscore, qn, (0, 0)).astype(BF16).astype(F32)
            dva[...] += dot(prob_b, dout, (0, 0)).astype(BF16).astype(F32)
            dq, term = norm_back(query_src, query_inv, qg, dqn)
            g[h, rows(j * back, block)] = dq.astype(BF16)
            gsum[0:1, :] += jnp.sum(term, axis=0, keepdims=True)
            return inner

        lax.fori_loop(0, n, one_block, 0)
        dk, term = norm_back(key_src, key_inv, kg, dka[...])
        gsum[1:2, :] += jnp.sum(term, axis=0, keepdims=True)
        for part, grad in ((1, dk.astype(BF16)), (2, dva[...].astype(BF16))):
            for j in range(n):
                start = j * back + part * block
                g[h, start:start + img] = grad[j * img:(j + 1) * img]
                g[h, start + img:start + block] = grad[image + j * txt:image + (j + 1) * txt]

        @pl.when(h < heads - 1)
        def _():
            send_back(h)

        keep_own(h)
        return carry

    lax.fori_loop(0, heads, head, 0)


    back_copy(heads - 1, cross_first(me, n, 0)).start()

    @pl.when(has_left)
    def _():
        pl.semaphore_wait(column.at[1], 1)

    partial = gsum[...]
    base = 0
    for stage, (stride, radix) in enumerate(stages):
        digit, others = peers(stage)
        slot = dpbuf.at[base + digit]
        slot[...] = partial
        for peer in others:
            pltpu.make_async_remote_copy(
                src_ref=slot, dst_ref=slot, send_sem=gs.at[stage], recv_sem=gr.at[stage],
                device_id={"dp": peer}, device_id_type=MESH,
            ).start()
        rest = dpbuf.at[pl.ds(base, radix - 1)]
        pltpu.make_async_copy(rest, rest, gr.at[stage]).wait()
        partial = jnp.sum(dpbuf[base:base + radix], axis=0)
        base += radix
    last = len(stages)
    sqbuf[me] = partial
    for i in range(n - 1):
        pltpu.make_async_remote_copy(
            src_ref=sqbuf.at[me], dst_ref=sqbuf.at[me], send_sem=gs.at[last], recv_sem=gr.at[last],
            device_id={"seq": cross_first(me, n, i)}, device_id_type=MESH,
        ).start()

    if heads > 1 and n > 2:
        back_copy(heads - 2, cross_first(me, n, 1)).start()

    for i in range(1, n - 1):
        back_copy(heads - 1, cross_first(me, n, i)).start()

    base = 0
    for stage, (stride, radix) in enumerate(stages):
        rest = dpbuf.at[pl.ds(base, radix - 1)]
        pltpu.make_async_copy(rest, rest, gs.at[stage]).wait()
        base += radix
    out = x.at[:, pl.ds(0, (n - 1) * heads * HEAD_DIM)]
    pltpu.make_async_copy(out, out, fs.at[0]).wait()
    rest = sqbuf.at[pl.ds(0, n - 1)]
    pltpu.make_async_copy(rest, rest, gr.at[last]).wait()
    pltpu.make_async_copy(rest, rest, gs.at[last]).wait()
    total[...] = jnp.sum(sqbuf[...], axis=0)
    out = y.at[:, pl.ds(0, (n - 1) * heads * HEAD_DIM)]
    pltpu.make_async_copy(out, out, bs.at[0]).wait()
    pltpu.make_async_copy(out, out, br.at[0]).wait()


def hand_on(y, total, *refs):
    grads, gains, sems = refs[:6], refs[6:8], refs[8]
    at = 0
    stores = []
    for out in grads:
        stores.append(pltpu.make_async_copy(y.at[pl.ds(at, out.shape[0])], out, sems.at[0]))
        at += out.shape[0]
    for i, out in enumerate(gains):
        stores.append(pltpu.make_async_copy(total.at[pl.ds(i, 1)], out, sems.at[1]))
    for store in stores:
        store.start()
    pltpu.make_async_copy(y, y, sems.at[0]).wait()
    pltpu.make_async_copy(total, total, sems.at[1]).wait()


def local(n, dp, iq, ik, iv, idt, tq, tk, tv, td, q_gain, k_gain):
    img, width = iq.shape[1:]
    txt, text = tq.shape[1], tk.shape[1]
    heads = width // HEAD_DIM // n
    keys = img * n + text
    block = img + txt
    sent, back = 2 * block + 2 * img, 3 * block
    stages = ladder(dp)
    vmem = pl.BlockSpec(memory_space=pltpu.VMEM)
    hbm = pl.BlockSpec(memory_space=pltpu.HBM)
    out = pl.pallas_call(
        functools.partial(kernel, n, dp, heads),
        out_shape=(
            jax.ShapeDtypeStruct((back, width), BF16),
            jax.ShapeDtypeStruct((2, HEAD_DIM), F32),
        ),
        in_specs=[hbm] * 10,
        out_specs=(vmem, vmem),
        scratch_shapes=[
            pltpu.VMEM((sent, width), BF16),
            pltpu.VMEM((text, width), BF16),
            pltpu.VMEM((text, width), BF16),
            pltpu.VMEM((2, HEAD_DIM), F32),
            pltpu.VMEM((heads, n * sent, HEAD_DIM), BF16),
            pltpu.VMEM((heads, n * back, HEAD_DIM), BF16),
            pltpu.VMEM((keys, HEAD_DIM), BF16),
            pltpu.VMEM((keys, HEAD_DIM), BF16),
            pltpu.VMEM((keys, HEAD_DIM), BF16),
            pltpu.VMEM((keys, HEAD_DIM), F32),
            pltpu.VMEM((keys, HEAD_DIM), F32),
            pltpu.VMEM((2, HEAD_DIM), F32),
            pltpu.VMEM((sum(radix for _, radix in stages), 2, HEAD_DIM), F32),
            pltpu.VMEM((n, 2, HEAD_DIM), F32),
            pltpu.SemaphoreType.DMA((4,)),
            pltpu.SemaphoreType.DMA((1,)),
            pltpu.SemaphoreType.DMA((heads,)),
            pltpu.SemaphoreType.DMA((1,)),
            pltpu.SemaphoreType.DMA((1,)),
            pltpu.SemaphoreType.DMA((len(stages) + 1,)),
            pltpu.SemaphoreType.DMA((len(stages) + 1,)),
            pltpu.SemaphoreType.REGULAR((2, n)),
            pltpu.SemaphoreType.REGULAR((2,)),
        ],
        compiler_params=pltpu.CompilerParams(
            collective_id=0, has_side_effects=True, vmem_limit_bytes=VMEM_LIMIT
        ),
    )(
        *(pltpu.with_memory_space_constraint(a, pltpu.HBM) for a in (
        iq[0], ik[0], iv[0], idt[0], tq[0], tk[0], tv[0], td[0],
        q_gain.reshape(1, HEAD_DIM), k_gain.reshape(1, HEAD_DIM)))
    )
    image, rest = (img, width), (txt, width)
    final = pl.pallas_call(
        hand_on,
        out_shape=tuple(jax.ShapeDtypeStruct(a, BF16) for a in (image, rest) * 3)
        + (jax.ShapeDtypeStruct((1, HEAD_DIM), F32),) * 2,
        in_specs=[vmem] * 2,
        out_specs=(hbm,) * 8,
        scratch_shapes=[pltpu.SemaphoreType.DMA((2,))],
        compiler_params=pltpu.CompilerParams(vmem_limit_bytes=VMEM_LIMIT),
    )(*out)
    order = (0, 2, 4, 1, 3, 5)
    return (*(final[i][None] for i in order), final[6][0], final[7][0])


def solution(mesh):
    split = P("dp", "seq", None)
    whole = P("dp", None, None)
    return jax.shard_map(
        functools.partial(local, mesh.shape["seq"], mesh.shape["dp"]),
        mesh=mesh,
        in_specs=(split, split, split, split, split, whole, whole, split, P(), P()),
        out_specs=(split,) * 6 + (P(), P()),
        check_vma=False,
    )
```

```python
import functools

import jax
import jax.numpy as jnp
from jax import lax
from jax.experimental import pallas as pl
from jax.experimental.pallas import tpu as pltpu
from jax.sharding import PartitionSpec as P

MESH = pl.DeviceIdType.MESH
HEAD_DIM = 128
EPSILON = 1e-06
VMEM_LIMIT = 24 * 1024 * 1024
F32 = jnp.float32
BF16 = jnp.bfloat16


def dot(a, b, contract):
    return lax.dot_general(a, b, ((contract[:1], contract[1:]), ((), ())), preferred_element_type=F32)


def inverse_rms(values):
    return lax.rsqrt(jnp.mean(values * values, axis=-1, keepdims=True) + EPSILON)


def norm_back(values, inverse, gain, upstream):
    unit = values * inverse
    lifted = upstream * gain
    mean = jnp.mean(lifted * unit, axis=-1, keepdims=True)
    return inverse * (lifted - unit * mean), upstream * unit


def ladder(dp):
    stages, stride = [], 1
    while stride < dp:
        left = dp // stride
        radix = max((r for r in range(2, 9) if left % r == 0), default=left)
        stages.append((stride, radix))
        stride *= radix
    return stages


def near_first(me, n, i):
    up = jnp.where(me + 1 + i < n, me + 1 + i, n - 2 - i)
    down = jnp.where(me - 1 - i >= 0, me - 1 - i, i + 1)
    return jnp.where(2 * me < n, up, down)


def cross_first(me, n, i):
    half = n // 2
    lower = me < half
    count = jnp.where(lower, n - half, half)
    own = jnp.where(lower, 0, half) + i - count
    return jnp.where(i < count, jnp.where(lower, half, 0) + i, jnp.where(own < me, own, own + 1))


def kernel(
    n, dp, heads,
    h_iq, h_ik, h_iv, h_idt, h_tq, h_tk, h_tv, h_td, h_qg, h_kg,
    y, total,
    x, gains, r, g, kc, vc, knb, dka, dva, gsum, dpbuf, sqbuf,
    ins, fs, fr, bs, br, gs, gr, tokens, column,
):
    me = lax.axis_index("seq")
    my_dp = lax.axis_index("dp")
    img, txt, text = h_iq.shape[0], h_tq.shape[0], h_tk.shape[0]
    block = img + txt
    sent = 2 * block + 2 * img
    back = 3 * block
    image = img * n
    stages = ladder(dp)
    has_left, has_right = me > 0, me < n - 1

    def col(owner, h):
        return pl.ds(pl.multiple_of((owner * heads + h) * HEAD_DIM, HEAD_DIM), HEAD_DIM)

    def rows(start, size):
        return pl.ds(pl.multiple_of(start, 16), size)

    def peers(stage):
        stride, radix = stages[stage]
        digit = lax.rem(lax.div(my_dp, stride), radix)
        return digit, [my_dp + (lax.rem(digit + s, radix) - digit) * stride for s in range(1, radix)]

    order = [near_first(me, n, i) for i in range(n - 1)]
    parts, at = [], 0
    for src, size in ((h_iq, img), (h_tq, txt), (h_ik, img), (h_iv, img), (h_idt, img), (h_td, txt)):
        parts.append((src, at, size))
        at += size
    loads = [pltpu.make_async_copy(src, x.at[pl.ds(at, size)], ins.at[0]) for src, at, size in parts]
    loads += [
        pltpu.make_async_copy(h_tk, x.at[pl.ds(sent, text)], ins.at[0]),
        pltpu.make_async_copy(h_tv, x.at[pl.ds(sent + text, text)], ins.at[0]),
        pltpu.make_async_copy(h_qg, gains.at[pl.ds(0, 1)], ins.at[1]),
        pltpu.make_async_copy(h_kg, gains.at[pl.ds(1, 1)], ins.at[1]),
    ]
    barrier = pltpu.get_barrier_semaphore()

    def tell(ref, axis, target):
        pl.semaphore_signal(ref, inc=1, device_id={axis: target}, device_id_type=MESH)

    def first_copy():
        for src, at, size in parts:
            pltpu.make_async_remote_copy(
                src_ref=src.at[:, col(order[0], 0)], dst_ref=r.at[0, rows(me * sent + at, size)],
                send_sem=fs.at[0], recv_sem=fr.at[0],
                device_id={"seq": order[0]}, device_id_type=MESH,
            ).start()

    def forward_copy(h, target):
        return pltpu.make_async_remote_copy(
            src_ref=x.at[pl.ds(0, sent), col(target, h)], dst_ref=r.at[h, rows(me * sent, sent)],
            send_sem=fs.at[0], recv_sem=fr.at[h],
            device_id={"seq": target}, device_id_type=MESH,
        )

    middle = n // 2 if n > 3 else n

    @pl.when(me == middle)
    def _():
        tell(barrier, "seq", me - 1)

    @pl.when(has_right)
    def _():
        tell(barrier, "seq", me + 1)

    @pl.when(has_left)
    def _():
        pl.semaphore_wait(barrier, jnp.where(me == middle - 1, 2, 1))

    @pl.when(has_left & (me != middle))
    def _():
        tell(tokens.at[0], "seq", me - 1)

    @pl.when(2 * me >= n)
    def _():
        first_copy()

    for load in loads:
        load.start()
    dp_peers = [peer for stage in range(len(stages)) for peer in peers(stage)[1]]

    @pl.when(me == 0)
    def _():
        for peer in dp_peers:
            tell(barrier, "dp", peer)

    for k in range(n - 1):
        @pl.when(me < n - 1 - k)
        def _():
            if k == 0:
                @pl.when(me != middle - 1)
                def _():
                    pl.semaphore_wait(tokens.at[0], 1)
            else:
                pl.semaphore_wait(tokens.at[k], 1)
            if k == 0:
                @pl.when(2 * me < n)
                def _():
                    first_copy()

                @pl.when(has_left)
                def _():
                    tell(tokens.at[n - 1], "seq", me + 1)

            if k < n - 2:
                @pl.when(has_left)
                def _():
                    tell(tokens.at[k + 1], "seq", me - 1)

    for k in range(n - 2):
        @pl.when(me > k + 1)
        def _():
            pl.semaphore_wait(tokens.at[n - 1 + k], 1)
            if k < n - 3:
                @pl.when(has_right)
                def _():
                    tell(tokens.at[n + k], "seq", me + 1)

    pltpu.make_async_copy(x, x, ins.at[0]).wait()
    for i in range(1, n - 1):
        forward_copy(0, order[i]).start()

    def send_head(h, carry):
        for i in range(n - 1):
            forward_copy(h, order[i]).start()
        return carry

    lax.fori_loop(1, heads, send_head, 0)

    @pl.when(me == 0)
    def _():
        pl.semaphore_wait(barrier, len(dp_peers))
        for peer in dp_peers:
            tell(column.at[0], "dp", peer)
        pl.semaphore_wait(column.at[0], len(dp_peers))
        for target in range(1, n):
            tell(column.at[1], "seq", target)

    def own_head(h, carry):
        r[h, rows(me * sent, sent)] = x[0:sent, col(me, h)]
        return carry

    lax.fori_loop(0, heads, own_head, 0)
    gsum[...] = jnp.zeros_like(gsum)
    pltpu.make_async_copy(gains, gains, ins.at[1]).wait()

    def back_copy(h, target):
        return pltpu.make_async_remote_copy(
            src_ref=g.at[h, rows(target * back, back)], dst_ref=y.at[:, col(me, h)],
            send_sem=bs.at[0], recv_sem=br.at[0],
            device_id={"seq": target}, device_id_type=MESH,
        )

    keep = (me == n - 1)

    def send_back(h):
        for i in range(n - 1):
            @pl.when((i != 1) | (h < heads - 2) | keep)
            def _():
                back_copy(h, cross_first(me, n, i)).start()

    def keep_own(h):
        y[:, col(me, h)] = g[h, rows(me * back, back)]

    qg = gains[0:1]
    kg = gains[1:2]
    scale = HEAD_DIM ** (-0.5)

    def head(h, carry):
        rest = r.at[h, pl.ds(0, (n - 1) * sent)]
        pltpu.make_async_copy(rest, rest, fr.at[h]).wait()
        for j in range(n):
            kc[j * img:(j + 1) * img] = r[h, j * sent + block:j * sent + block + img]
            vc[j * img:(j + 1) * img] = r[h, j * sent + block + img:j * sent + block + 2 * img]
        kc[image:image + text] = x[sent:sent + text, col(me, h)]
        vc[image:image + text] = x[sent + text:sent + 2 * text, col(me, h)]
        key_src = kc[...].astype(F32)
        key_inv = inverse_rms(key_src)
        knb[...] = (key_src * key_inv * kg).astype(BF16)
        dka[...] = jnp.zeros_like(dka)
        dva[...] = jnp.zeros_like(dva)

        def one_block(j, inner):
            query_src = r[h, rows(j * sent, block)].astype(F32)
            query_inv = inverse_rms(query_src)
            qn = (query_src * query_inv * qg).astype(BF16)
            kn = knb[...]
            value = vc[...]
            dout = r[h, rows(j * sent + block + 2 * img, block)]
            scores = dot(qn, kn, (1, 1)) * scale
            exps = jnp.exp(scores - jnp.max(scores, axis=-1, keepdims=True))
            prob = exps * (1.0 / jnp.sum(exps, axis=-1, keepdims=True))
            prob_b = prob.astype(BF16)
            output = dot(prob_b, value, (1, 0)).astype(BF16)
            dprob = dot(dout, value, (1, 1))
            delta = jnp.sum(dout.astype(F32) * output.astype(F32), axis=-1, keepdims=True)
            dscore = (prob * (dprob - delta) * scale).astype(BF16)
            dqn = dot(dscore, kn, (1, 0))
            dka[...] += dot(dscore, qn, (0, 0)).astype(BF16).astype(F32)
            dva[...] += dot(prob_b, dout, (0, 0)).astype(BF16).astype(F32)
            dq, term = norm_back(query_src, query_inv, qg, dqn)
            g[h, rows(j * back, block)] = dq.astype(BF16)
            gsum[0:1, :] += jnp.sum(term, axis=0, keepdims=True)
            return inner

        lax.fori_loop(0, n, one_block, 0)
        dk, term = norm_back(key_src, key_inv, kg, dka[...])
        gsum[1:2, :] += jnp.sum(term, axis=0, keepdims=True)
        for part, grad in ((1, dk.astype(BF16)), (2, dva[...].astype(BF16))):
            for j in range(n):
                start = j * back + part * block
                g[h, start:start + img] = grad[j * img:(j + 1) * img]
                g[h, start + img:start + block] = grad[image + j * txt:image + (j + 1) * txt]

        @pl.when(h < heads - 1)
        def _():
            send_back(h)

        keep_own(h)
        return carry

    lax.fori_loop(0, heads, head, 0)


    back_copy(heads - 1, cross_first(me, n, 0)).start()

    @pl.when(has_left)
    def _():
        pl.semaphore_wait(column.at[1], 1)

    partial = gsum[...]
    base = 0
    for stage, (stride, radix) in enumerate(stages):
        digit, others = peers(stage)
        slot = dpbuf.at[base + digit]
        slot[...] = partial
        for peer in others:
            pltpu.make_async_remote_copy(
                src_ref=slot, dst_ref=slot, send_sem=gs.at[stage], recv_sem=gr.at[stage],
                device_id={"dp": peer}, device_id_type=MESH,
            ).start()
        rest = dpbuf.at[pl.ds(base, radix - 1)]
        pltpu.make_async_copy(rest, rest, gr.at[stage]).wait()
        partial = jnp.sum(dpbuf[base:base + radix], axis=0)
        base += radix
    last = len(stages)
    sqbuf[me] = partial
    for i in range(n - 1):
        pltpu.make_async_remote_copy(
            src_ref=sqbuf.at[me], dst_ref=sqbuf.at[me], send_sem=gs.at[last], recv_sem=gr.at[last],
            device_id={"seq": cross_first(me, n, i)}, device_id_type=MESH,
        ).start()

    if heads > 1 and n > 2:
        @pl.when(jnp.logical_not(keep))
        def _():
            back_copy(heads - 2, cross_first(me, n, 1)).start()

    for i in range(1, n - 1):
        back_copy(heads - 1, cross_first(me, n, i)).start()

    base = 0
    for stage, (stride, radix) in enumerate(stages):
        rest = dpbuf.at[pl.ds(base, radix - 1)]
        pltpu.make_async_copy(rest, rest, gs.at[stage]).wait()
        base += radix
    out = x.at[pl.ds(0, sent), pl.ds(0, (n - 1) * heads * HEAD_DIM)]
    pltpu.make_async_copy(out, out, fs.at[0]).wait()
    rest = sqbuf.at[pl.ds(0, n - 1)]
    pltpu.make_async_copy(rest, rest, gr.at[last]).wait()
    pltpu.make_async_copy(rest, rest, gs.at[last]).wait()
    total[...] = jnp.sum(sqbuf[...], axis=0)
    out = y.at[:, pl.ds(0, (n - 1) * heads * HEAD_DIM)]
    pltpu.make_async_copy(out, out, bs.at[0]).wait()
    pltpu.make_async_copy(out, out, br.at[0]).wait()


def hand_on(y, total, *refs):
    grads, gains, sems = refs[:6], refs[6:8], refs[8]
    at = 0
    stores = []
    for out in grads:
        stores.append(pltpu.make_async_copy(y.at[pl.ds(at, out.shape[0])], out, sems.at[0]))
        at += out.shape[0]
    for i, out in enumerate(gains):
        stores.append(pltpu.make_async_copy(total.at[pl.ds(i, 1)], out, sems.at[1]))
    for store in stores:
        store.start()
    pltpu.make_async_copy(y, y, sems.at[0]).wait()
    pltpu.make_async_copy(total, total, sems.at[1]).wait()


def local(n, dp, iq, ik, iv, idt, tq, tk, tv, td, q_gain, k_gain):
    img, width = iq.shape[1:]
    txt, text = tq.shape[1], tk.shape[1]
    heads = width // HEAD_DIM // n
    keys = img * n + text
    block = img + txt
    sent, back = 2 * block + 2 * img, 3 * block
    stages = ladder(dp)
    vmem = pl.BlockSpec(memory_space=pltpu.VMEM)
    hbm = pl.BlockSpec(memory_space=pltpu.HBM)
    out = pl.pallas_call(
        functools.partial(kernel, n, dp, heads),
        out_shape=(
            jax.ShapeDtypeStruct((back, width), BF16),
            jax.ShapeDtypeStruct((2, HEAD_DIM), F32),
        ),
        in_specs=[hbm] * 10,
        out_specs=(vmem, vmem),
        scratch_shapes=[
            pltpu.VMEM((sent + 2 * text, width), BF16),
            pltpu.VMEM((2, HEAD_DIM), F32),
            pltpu.VMEM((heads, n * sent, HEAD_DIM), BF16),
            pltpu.VMEM((heads, n * back, HEAD_DIM), BF16),
            pltpu.VMEM((keys, HEAD_DIM), BF16),
            pltpu.VMEM((keys, HEAD_DIM), BF16),
            pltpu.VMEM((keys, HEAD_DIM), BF16),
            pltpu.VMEM((keys, HEAD_DIM), F32),
            pltpu.VMEM((keys, HEAD_DIM), F32),
            pltpu.VMEM((2, HEAD_DIM), F32),
            pltpu.VMEM((sum(radix for _, radix in stages), 2, HEAD_DIM), F32),
            pltpu.VMEM((n, 2, HEAD_DIM), F32),
            pltpu.SemaphoreType.DMA((2,)),
            pltpu.SemaphoreType.DMA((1,)),
            pltpu.SemaphoreType.DMA((heads,)),
            pltpu.SemaphoreType.DMA((1,)),
            pltpu.SemaphoreType.DMA((1,)),
            pltpu.SemaphoreType.DMA((len(stages) + 1,)),
            pltpu.SemaphoreType.DMA((len(stages) + 1,)),
            pltpu.SemaphoreType.REGULAR((2 * n - 3,)),
            pltpu.SemaphoreType.REGULAR((2,)),
        ],
        compiler_params=pltpu.CompilerParams(
            collective_id=0, has_side_effects=True, vmem_limit_bytes=VMEM_LIMIT
        ),
    )(
        *(pltpu.with_memory_space_constraint(a, pltpu.HBM) for a in (
        iq[0], ik[0], iv[0], idt[0], tq[0], tk[0], tv[0], td[0],
        q_gain.reshape(1, HEAD_DIM), k_gain.reshape(1, HEAD_DIM)))
    )
    image, rest = (img, width), (txt, width)
    final = pl.pallas_call(
        hand_on,
        out_shape=tuple(jax.ShapeDtypeStruct(a, BF16) for a in (image, rest) * 3)
        + (jax.ShapeDtypeStruct((1, HEAD_DIM), F32),) * 2,
        in_specs=[vmem] * 2,
        out_specs=(hbm,) * 8,
        scratch_shapes=[pltpu.SemaphoreType.DMA((2,))],
        compiler_params=pltpu.CompilerParams(vmem_limit_bytes=VMEM_LIMIT),
    )(*out)
    order = (0, 2, 4, 1, 3, 5)
    return (*(final[i][None] for i in order), final[6][0], final[7][0])


def solution(mesh):
    split = P("dp", "seq", None)
    whole = P("dp", None, None)
    return jax.shard_map(
        functools.partial(local, mesh.shape["seq"], mesh.shape["dp"]),
        mesh=mesh,
        in_specs=(split, split, split, split, split, whole, whole, split, P(), P()),
        out_specs=(split,) * 6 + (P(), P()),
        check_vma=False,
    )
```
